32 devices in a mesh: blk: 16 (over z, y, core), head: 2 (over x).
Axes of the slice: x: 2, y: 2, z: 4, core: 2. Of those that a mesh axis runs over, the one named last changes fastest.
Arguments:
- queries: bfloat16 [4096, 1024], P('blk', 'head'), may hold values from -216 to 216
- keys: bfloat16 [4096, 1024], P('blk', 'head'), may hold values from -6 to 6
- values: bfloat16 [4096, 1024], P('blk', 'head'), may hold values from -6 to 6
- group_table: int32 [16, 2], P('blk'), may hold values from 0 to 31, as said below
- doc_ids: int32 [4096], replicated, may hold values from 0 to 15, never falling along the last dimension, each value on 1 to 2048 neighbouring positions
Outputs:
- attended: bfloat16 [4096, 1024], P('blk', 'head')
The draws below stay inside these ranges and needn't reach their ends.
Inputs may be any that keep to these rules, and one draw needn't show every extreme that they name: group_table[d, 1] = 31 - group_table[d, 0]; the first column holds each of 0 to 15 once. `doc_ids`: document numbers never fall along positions; a document holds at most 2048 positions.
All inputs are finite; a program needn't handle non-finite values.
Results may differ from the reference program's by a relative error of at most 0.0049.
Values may be sent and summed in bfloat16 or wider, within the bound.
No kernel may reach another device: no remote copies, remote signals or barrier semaphores. Data moves between devices by JAX's collectives and lax.ppermute only.
A program may use at most 192 MiB of HBM per device.

```python
import math
import jax
import jax.numpy as jnp
import numpy as np
from jax import lax

HEAD_DIM = 128
HEADS = 8
TOK_DEV = 256
DOCS = 16
GROUP = 128
SEQ = 4096
MAXDOC = 2048
N_BLK = 16


def draw_queries(key, part):
    drawn = jnp.clip(jax.random.normal(jax.random.fold_in(key, 11), (SEQ, HEADS, HEAD_DIM), jnp.float32), -6.0, 6.0)
    return drawn.reshape(SEQ, HEADS * HEAD_DIM).astype(jnp.bfloat16)


def draw_keys(key, part):
    drawn = jnp.clip(jax.random.normal(jax.random.fold_in(key, 13), (SEQ, HEADS, HEAD_DIM), jnp.float32), -6.0, 6.0)
    return drawn.reshape(SEQ, HEADS * HEAD_DIM).astype(jnp.bfloat16)


def draw_group_table(key, part):
    order = jax.random.permutation(jax.random.fold_in(key, 17), N_BLK).astype(jnp.int32)
    return jnp.stack([order, 2 * N_BLK - 1 - order], axis=1).astype(jnp.int32)


def steps_of(key, extent, pieces, low, high):
    def one(dim, shards_of):
        heights = jax.random.uniform(jax.random.fold_in(jax.random.fold_in(key, 6), dim), (shards_of,), jnp.float32, low / len(pieces), high / len(pieces))
        return jnp.repeat(jnp.exp(heights), extent[dim] // shards_of).reshape((-1,) + (1,) * (len(extent) - dim - 1))

    loudness = one(*pieces[0])
    for cut in pieces[1:]:
        loudness = loudness * one(*cut)
    return loudness


def length_profile(amount, total, most, slope):
    loads = [(1 << 20) // math.isqrt(grade ** slope) + 1 for grade in range(2, amount + 1)]
    surplus, holding = total - most - (amount - 1), [1] * (amount - 1)
    while surplus > 0:
        candidates = [i for i in range(amount - 1) if holding[i] < most]
        whole, remaining = sum([loads[i] for i in candidates]), surplus
        for i in candidates:
            extra = min(most - holding[i], max(1, remaining * loads[i] // whole), surplus)
            holding[i] = holding[i] + extra
            surplus = surplus - extra
    return np.array([most] + holding)


def uneven(stream_key, count, total, most, slope):
    if count == 2:
        one = jax.random.randint(stream_key, (), max(1, total - most), min(most, total - 1) + 1)
        return jnp.stack([one, total - one])
    tallies = jnp.asarray(length_profile(count, total, most, slope), jnp.int32)
    twos = (count - 1) // 2
    donor, taker = tallies[1:1 + 2 * twos:2], tallies[2:2 + 2 * twos:2]
    margin = jnp.minimum(donor - 1, most - taker)
    passed = jax.random.randint(jax.random.fold_in(stream_key, 1), (twos,), 0, 1 << 20) % (margin + 1)
    tallies = tallies.at[1:1 + 2 * twos:2].set(donor - passed).at[2:2 + 2 * twos:2].set(taker + passed)
    return tallies[jax.random.permutation(jax.random.fold_in(stream_key, 2), count)]


def noise(rng, extent, deviation, reach, pieces=(), kind=jnp.bfloat16):
    values = jax.random.normal(rng, extent, jnp.float32) * deviation
    if len(pieces) > 0:
        values = steps_of(rng, extent, pieces, -0.22, 0.18) * values
    return jnp.clip(values, min=-reach, max=reach).astype(kind)


def setup_inputs(seed: int = 0) -> dict:
    streams_of = jax.random.split(jax.random.key(seed), 6)
    return {
        "queries": draw_queries(jax.random.fold_in(streams_of[5], 71), 0),
        "keys": draw_keys(jax.random.fold_in(streams_of[5], 71), 0),
        "values": noise(streams_of[2], (SEQ, HEADS * HEAD_DIM), 1.0, 6.0, ((0, 16), (1, 2))),
        "group_table": draw_group_table(jax.random.fold_in(streams_of[5], 71), 0),
        "doc_ids": jnp.searchsorted(jnp.cumsum(uneven(streams_of[4], DOCS, SEQ, MAXDOC, 2)), jnp.arange(SEQ), side="right").astype(jnp.int32),
    }


def reference(queries, keys, values, group_table, doc_ids):
    row_ids = jnp.arange(SEQ, dtype=jnp.int32)
    device = row_ids // TOK_DEV
    slot_ids = row_ids % TOK_DEV // GROUP
    position = (group_table[device, slot_ids] * GROUP + row_ids % GROUP).astype(jnp.int32)
    document = doc_ids[position]
    score_scale = 1.0 / math.sqrt(HEAD_DIM)
    query_block = math.gcd(SEQ, 1024)
    block_count = SEQ // query_block

    def one_head(head_index):
        start = (head_index * HEAD_DIM).astype(jnp.int32)
        head_queries = lax.dynamic_slice_in_dim(queries, start, HEAD_DIM, 1)
        head_keys = lax.dynamic_slice_in_dim(keys, start, HEAD_DIM, 1)
        head_values = lax.dynamic_slice_in_dim(values, start, HEAD_DIM, 1)

        def attend_block(args):
            query_rows, block_pos, block_doc = args
            scores = jnp.dot(query_rows, head_keys.T, preferred_element_type=jnp.float32) * score_scale
            visible = (block_doc[:, None] == document[None, :]) & (position[None, :] <= block_pos[:, None])
            rowmax = lax.optimization_barrier(jnp.max(jnp.where(visible, scores, -jnp.inf), axis=1))
            weights = jnp.where(visible, jnp.exp(scores - rowmax[:, None]), 0.0)
            denominator = lax.optimization_barrier(jnp.sum(weights, axis=1))
            output = jnp.dot(weights.astype(jnp.bfloat16), head_values, preferred_element_type=jnp.float32)
            return output / denominator[:, None]
        blocks = (head_queries.reshape(block_count, query_block, HEAD_DIM), position.reshape(block_count, query_block), document.reshape(block_count, query_block))
        return lax.map(attend_block, blocks).reshape(SEQ, HEAD_DIM)
    outputs = lax.map(one_head, jnp.arange(HEADS, dtype=jnp.int32))
    return jnp.transpose(outputs, (1, 0, 2)).reshape(SEQ, HEADS * HEAD_DIM).astype(jnp.bfloat16)
```

```python
import functools
import math

import jax
import jax.numpy as jnp
from jax import lax
from jax.experimental import pallas as pl
from jax.experimental.pallas import tpu as pltpu
from jax.sharding import PartitionSpec as P

HEAD_DIM = 128
CHUNK = 512
HIDDEN = -1e30


def attend_kernel(n_hi, n_lo, group, me_ref, table_ref, first_ref, start_ref, *refs):
    q_refs = refs[:n_hi]
    kv_refs = refs[n_hi:n_hi + n_lo]
    out_ref, key_buf, value_buf, score_buf = refs[n_hi + n_lo:]
    me = me_ref[0]
    factor = math.log2(math.e) / math.sqrt(HEAD_DIM)
    key_buf[:CHUNK] = jnp.zeros((CHUNK, HEAD_DIM), key_buf.dtype)
    value_buf[:CHUNK] = jnp.zeros((CHUNK, HEAD_DIM), value_buf.dtype)
    for lo in range(n_lo):
        for hi in range(n_hi):
            for slot in range(2):
                at = table_ref[me ^ (hi * n_lo + lo), slot] * group + CHUNK
                at = pl.multiple_of(at, group)
                rows = pl.ds(slot * group, group)
                key_buf[pl.ds(at, group)] = kv_refs[lo][hi, 0, rows]
                value_buf[pl.ds(at, group)] = kv_refs[lo][hi, 1, rows]

    lane = lax.broadcasted_iota(jnp.int32, (group, CHUNK), 1)
    row = lax.broadcasted_iota(jnp.int32, (group, CHUNK), 0)
    lanes = CHUNK // HEAD_DIM

    def by_lane(op, x):
        total = x[:, :HEAD_DIM]
        for i in range(1, lanes):
            total = op(total, x[:, i * HEAD_DIM:(i + 1) * HEAD_DIM])
        return total

    for hi in range(n_hi):
        for slot in range(2):
            number = table_ref[me ^ (hi * n_lo), slot]
            end = (number + 1) * group
            count = (end - first_ref[number] + CHUNK - 1) // CHUNK
            query = q_refs[hi][slot * group:(slot + 1) * group, :]
            starts = jnp.broadcast_to(start_ref[pl.ds(number, 1), :], (group, group)).T[:, :1]
            low = starts - lane
            high = row - lane + (end - group)

            def score(i, top):
                base = end - (i + 1) * CHUNK
                at = pl.multiple_of(base + CHUNK, group)
                s = lax.dot_general(
                    query, key_buf[pl.ds(at, CHUNK)],
                    (((1,), (1,)), ((), ())), preferred_element_type=jnp.float32,
                )
                s = jnp.where((low <= base) & (high >= base), s, HIDDEN)
                score_buf[i] = s
                return jnp.maximum(top, by_lane(jnp.maximum, s))

            top = lax.fori_loop(0, count, score, jnp.full((group, HEAD_DIM), HIDDEN, jnp.float32))
            top = jnp.max(top, axis=1, keepdims=True)

            def weigh(i, state):
                total, summed = state
                at = pl.multiple_of(end - i * CHUNK, group)
                w = jnp.exp2((score_buf[i] - top) * factor)
                total = total + by_lane(jnp.add, w)
                summed = summed + jnp.dot(
                    w.astype(jnp.bfloat16), value_buf[pl.ds(at, CHUNK)],
                    preferred_element_type=jnp.float32,
                )
                return total, summed

            zeros = jnp.zeros((group, HEAD_DIM), jnp.float32)
            total, summed = lax.fori_loop(0, count, weigh, (zeros, zeros))
            total = jnp.sum(total, axis=1, keepdims=True)
            out_ref[hi, slot * group:(slot + 1) * group, :] = (summed / total).astype(out_ref.dtype)


def shards(n_blk, queries, keys, values, group_table, doc_ids):
    tok_rows = queries.shape[0]
    group = tok_rows // 2
    n_hi = queries.shape[1] // HEAD_DIM
    n_lo = n_blk // n_hi
    seq = doc_ids.shape[0]
    me = lax.axis_index("blk")
    my_hi = me // n_lo

    def swap(x, by):
        return lax.ppermute(x, "blk", [(b, b ^ by) for b in range(n_blk)])

    def head_of(x, hi):
        return lax.dynamic_slice(x, (0, hi * HEAD_DIM), (tok_rows, HEAD_DIM))

    pieces = []
    for step in range(n_hi):
        piece = jnp.stack([head_of(x, my_hi ^ step) for x in (keys, values, queries)])
        pieces.append(swap(piece, step * n_lo) if step else piece)
    own = jnp.stack([piece[:2] for piece in pieces])
    held = {0: own}
    bit = n_lo // 2
    while bit:
        for j in list(held):
            held[j ^ bit] = swap(held[j], bit)
        bit //= 2

    table = lax.all_gather(group_table, "blk", axis=0, tiled=True)
    index = jnp.arange(seq, dtype=jnp.int32)
    before = jnp.concatenate([doc_ids[:1], doc_ids[:-1]])
    start = lax.cummax(jnp.where(doc_ids != before, index, 0))
    start = start.reshape(seq // group, group)

    smem = pl.BlockSpec(memory_space=pltpu.SMEM)
    vmem = pl.BlockSpec(memory_space=pltpu.VMEM)
    outs = pl.pallas_call(
        functools.partial(attend_kernel, n_hi, n_lo, group),
        out_shape=jax.ShapeDtypeStruct((n_hi, tok_rows, HEAD_DIM), jnp.bfloat16),
        in_specs=[smem] * 3 + [vmem] * (1 + n_hi + n_lo),
        out_specs=vmem,
        scratch_shapes=[
            pltpu.VMEM((seq + CHUNK, HEAD_DIM), jnp.bfloat16),
            pltpu.VMEM((seq + CHUNK, HEAD_DIM), jnp.bfloat16),
            pltpu.VMEM((seq // CHUNK, group, CHUNK), jnp.float32),
        ],
        name="attend",
    )(
        me.reshape(1), table, start[:, 0], start,
        *[piece[2] for piece in pieces], *[held[j] for j in range(n_lo)],
    )
    back = jnp.stack([swap(outs[j], j * n_lo) if j else outs[0] for j in range(n_hi)])
    heads = [lax.dynamic_index_in_dim(back, my_hi ^ h, 0, keepdims=False) for h in range(n_hi)]
    return jnp.concatenate(heads, axis=1)


def solution(mesh):
    in_specs = (P("blk", "head"), P("blk", "head"), P("blk", "head"), P("blk", None), P())
    out_specs = P("blk", "head")
    body = functools.partial(shards, mesh.shape["blk"])
    return jax.shard_map(body, mesh=mesh, in_specs=in_specs, out_specs=out_specs, check_vma=False)
```

```python
import functools
import math

import jax
import jax.numpy as jnp
from jax import lax
from jax.experimental import pallas as pl
from jax.experimental.pallas import tpu as pltpu
from jax.sharding import PartitionSpec as P

HEAD_DIM = 128
CHUNK = 512
HIDDEN = -1e30
NOTE_ROWS = 16


def attend_kernel(n_hi, n_lo, group, first_ref, start_ref, *refs):
    tok_rows = 2 * group
    piece_refs = refs[:n_hi]
    held_refs = refs[n_hi:n_hi + n_lo - 1]
    out_refs = refs[n_hi + n_lo - 1:2 * n_hi + n_lo - 1]
    key_buf, value_buf, score_buf = refs[2 * n_hi + n_lo - 1:]
    factor = math.log2(math.e) / math.sqrt(HEAD_DIM)

    def stored(hi, lo, first, count):
        rows = slice(first, first + count)
        return held_refs[lo - 1][hi, rows] if lo else piece_refs[hi][rows]

    def group_numbers(hi, lo):
        notes = stored(hi, lo, 2 * tok_rows, NOTE_ROWS).astype(jnp.float32).astype(jnp.int32)
        return notes[0, 0], notes[NOTE_ROWS // 2, 0]

    key_buf[:CHUNK] = jnp.zeros((CHUNK, HEAD_DIM), key_buf.dtype)
    value_buf[:CHUNK] = jnp.zeros((CHUNK, HEAD_DIM), value_buf.dtype)
    mine = []
    for lo in range(n_lo):
        for hi in range(n_hi):
            numbers = group_numbers(hi, lo)
            if lo == 0:
                mine.append(numbers)
            for slot in range(2):
                at = pl.multiple_of(numbers[slot] * group + CHUNK, group)
                key_buf[pl.ds(at, group)] = stored(hi, lo, slot * group, group)
                value_buf[pl.ds(at, group)] = stored(hi, lo, tok_rows + slot * group, group)

    lane = lax.broadcasted_iota(jnp.int32, (group, CHUNK), 1)
    row = lax.broadcasted_iota(jnp.int32, (group, CHUNK), 0)
    lanes = CHUNK // HEAD_DIM

    def by_lane(op, x):
        total = x[:, :HEAD_DIM]
        for i in range(1, lanes):
            total = op(total, x[:, i * HEAD_DIM:(i + 1) * HEAD_DIM])
        return total

    for hi in range(n_hi):
        for slot in range(2):
            number = mine[hi][slot]
            end = (number + 1) * group
            count = (end - first_ref[number] + CHUNK - 1) // CHUNK
            q_row = 2 * tok_rows + NOTE_ROWS + slot * group
            query = piece_refs[hi][q_row:q_row + group, :]
            starts = jnp.broadcast_to(start_ref[pl.ds(number, 1), :], (group, group)).T[:, :1]
            low = starts - lane
            high = row - lane + (end - group)

            def score(i, top):
                base = end - (i + 1) * CHUNK
                at = pl.multiple_of(base + CHUNK, group)
                s = lax.dot_general(
                    query, key_buf[pl.ds(at, CHUNK)],
                    (((1,), (1,)), ((), ())), preferred_element_type=jnp.float32,
                )
                s = jnp.where((low <= base) & (high >= base), s, HIDDEN)
                score_buf[i] = s
                return jnp.maximum(top, by_lane(jnp.maximum, s))

            top = lax.fori_loop(0, count, score, jnp.full((group, HEAD_DIM), HIDDEN, jnp.float32))
            top = jnp.max(top, axis=1, keepdims=True)

            def weigh(i, state):
                total, summed = state
                at = pl.multiple_of(end - i * CHUNK, group)
                w = jnp.exp2((score_buf[i] - top) * factor)
                total = total + by_lane(jnp.add, w)
                summed = summed + jnp.dot(
                    w.astype(jnp.bfloat16), value_buf[pl.ds(at, CHUNK)],
                    preferred_element_type=jnp.float32,
                )
                return total, summed

            zeros = jnp.zeros((group, HEAD_DIM), jnp.float32)
            total, summed = lax.fori_loop(0, count, weigh, (zeros, zeros))
            total = jnp.sum(total, axis=1, keepdims=True)
            out_refs[hi][slot * group:(slot + 1) * group, :] = (summed / total).astype(jnp.bfloat16)


def shards(n_blk, queries, keys, values, group_table, doc_ids):
    tok_rows = queries.shape[0]
    group = tok_rows // 2
    n_hi = queries.shape[1] // HEAD_DIM
    n_lo = n_blk // n_hi
    seq = doc_ids.shape[0]
    assert seq // group <= 256
    me = lax.axis_index("blk")
    my_hi = me // n_lo

    def swap(x, by):
        return lax.ppermute(x, "blk", [(b, b ^ by) for b in range(n_blk)])

    def head_of(x, hi):
        return lax.dynamic_slice(x, (0, hi * HEAD_DIM), (tok_rows, HEAD_DIM))

    notes = jnp.repeat(group_table[0], NOTE_ROWS // 2).astype(jnp.bfloat16)
    notes = jnp.broadcast_to(notes[:, None], (NOTE_ROWS, HEAD_DIM))
    kv_rows = 2 * tok_rows + NOTE_ROWS
    pieces = []
    for step in range(n_hi):
        hi = my_hi ^ step
        piece = jnp.concatenate([head_of(keys, hi), head_of(values, hi), notes, head_of(queries, hi)])
        pieces.append(swap(piece, step * n_lo) if step else piece)
    own = jnp.stack([piece[:kv_rows] for piece in pieces])
    held = {0: own}
    bit = n_lo // 2
    while bit:
        for j in list(held):
            held[j ^ bit] = swap(held[j], bit)
        bit //= 2

    index = jnp.arange(seq, dtype=jnp.int32)
    before = jnp.concatenate([doc_ids[:1], doc_ids[:-1]])
    start = lax.cummax(jnp.where(doc_ids != before, index, 0))
    start = start.reshape(seq // group, group)

    smem = pl.BlockSpec(memory_space=pltpu.SMEM)
    vmem = pl.BlockSpec(memory_space=pltpu.VMEM)
    outs = pl.pallas_call(
        functools.partial(attend_kernel, n_hi, n_lo, group),
        out_shape=[jax.ShapeDtypeStruct((tok_rows, HEAD_DIM), jnp.bfloat16)] * n_hi,
        in_specs=[smem] + [vmem] * (n_hi + n_lo),
        out_specs=[vmem] * n_hi,
        scratch_shapes=[
            pltpu.VMEM((seq + CHUNK, HEAD_DIM), jnp.bfloat16),
            pltpu.VMEM((seq + CHUNK, HEAD_DIM), jnp.bfloat16),
            pltpu.VMEM((seq // CHUNK, group, CHUNK), jnp.float32),
        ],
        name="attend",
    )(
        start[:, 0], start, *pieces, *[held[j] for j in range(1, n_lo)],
    )
    back = jnp.stack([swap(outs[j], j * n_lo) if j else outs[0] for j in range(n_hi)])
    heads = [lax.dynamic_index_in_dim(back, my_hi ^ h, 0, keepdims=False) for h in range(n_hi)]
    return jnp.concatenate(heads, axis=1)


def solution(mesh):
    in_specs = (P("blk", "head"), P("blk", "head"), P("blk", "head"), P("blk", None), P())
    out_specs = P("blk", "head")
    body = functools.partial(shards, mesh.shape["blk"])
    return jax.shard_map(body, mesh=mesh, in_specs=in_specs, out_specs=out_specs, check_vma=False)
```

```python
import functools
import math

import jax
import jax.numpy as jnp
from jax import lax
from jax.experimental import pallas as pl
from jax.experimental.pallas import tpu as pltpu
from jax.sharding import PartitionSpec as P

HEAD_DIM = 128
CHUNK = 512
HIDDEN = -1e30
NOTE_ROWS = 16
PAIR = 4


def attend_kernel(n_hi, n_lo, group, first_ref, start_ref, *refs):
    tok_rows = 2 * group
    piece_refs = refs[:n_hi]
    n_held = 2 * (n_lo - 1)
    held_refs = refs[n_hi:n_hi + n_held]
    out_refs = refs[n_hi + n_held:2 * n_hi + n_held]
    key_buf, value_buf, score_buf = refs[2 * n_hi + n_held:]
    half = 2
    factor = math.log2(math.e) / math.sqrt(HEAD_DIM)

    def stored(hi, lo, first, count):
        rows = slice(first, first + count)
        if lo == 0:
            return piece_refs[hi][rows]
        return held_refs[hi // half * (n_lo - 1) + lo - 1][hi % half, rows]

    def group_numbers(hi, lo):
        notes = stored(hi, lo, 2 * tok_rows, NOTE_ROWS).astype(jnp.float32).astype(jnp.int32)
        return notes[0, 0], notes[NOTE_ROWS // 2, 0]

    key_buf[:CHUNK] = jnp.zeros((CHUNK, HEAD_DIM), key_buf.dtype)
    value_buf[:CHUNK] = jnp.zeros((CHUNK, HEAD_DIM), value_buf.dtype)
    mine = []
    for lo in range(n_lo):
        for hi in range(n_hi):
            numbers = group_numbers(hi, lo)
            if lo == 0:
                mine.append(numbers)
            for slot in range(2):
                at = pl.multiple_of(numbers[slot] * group + CHUNK, group)
                key_buf[pl.ds(at, group)] = stored(hi, lo, slot * group, group)
                value_buf[pl.ds(at, group)] = stored(hi, lo, tok_rows + slot * group, group)

    lane = lax.broadcasted_iota(jnp.int32, (group, CHUNK), 1)
    row = lax.broadcasted_iota(jnp.int32, (group, CHUNK), 0)
    lanes = CHUNK // HEAD_DIM

    def by_lane(op, x):
        total = x[:, :HEAD_DIM]
        for i in range(1, lanes):
            total = op(total, x[:, i * HEAD_DIM:(i + 1) * HEAD_DIM])
        return total

    def attend(tasks):
        ends, lows, highs, queries = [], [], [], []
        count = 0
        for hi, slot in tasks:
            number = mine[hi][slot]
            end = (number + 1) * group
            count = jnp.maximum(count, (end - first_ref[number] + CHUNK - 1) // CHUNK)
            q_row = 2 * tok_rows + NOTE_ROWS + slot * group
            starts = jnp.broadcast_to(start_ref[pl.ds(number, 1), :], (group, group)).T[:, :1]
            ends.append(end)
            lows.append(starts - lane)
            highs.append(row - lane + (end - group))
            queries.append(piece_refs[hi][q_row:q_row + group, :])
        n = len(tasks)

        def rows_at(i, t):
            base = ends[t] - (i + 1) * CHUNK
            return base, pl.multiple_of(jnp.maximum(base + CHUNK, 0), group)

        def score(i, tops):
            out = []
            for t in range(n):
                base, at = rows_at(i, t)
                s = lax.dot_general(
                    queries[t], key_buf[pl.ds(at, CHUNK)],
                    (((1,), (1,)), ((), ())), preferred_element_type=jnp.float32,
                )
                s = jnp.where((lows[t] <= base) & (highs[t] >= base), s, HIDDEN)
                score_buf[t, i] = s
                out.append(jnp.maximum(tops[t], by_lane(jnp.maximum, s)))
            return tuple(out)

        hidden = jnp.full((group, HEAD_DIM), HIDDEN, jnp.float32)
        tops = lax.fori_loop(0, count, score, (hidden,) * n)
        tops = [jnp.max(top, axis=1, keepdims=True) for top in tops]

        def weigh(i, state):
            out = []
            for t in range(n):
                total, summed = state[t]
                _, at = rows_at(i, t)
                w = jnp.exp2((score_buf[t, i] - tops[t]) * factor)
                total = total + by_lane(jnp.add, w)
                summed = summed + jnp.dot(
                    w.astype(jnp.bfloat16), value_buf[pl.ds(at, CHUNK)],
                    preferred_element_type=jnp.float32,
                )
                out.append((total, summed))
            return tuple(out)

        zeros = jnp.zeros((group, HEAD_DIM), jnp.float32)
        state = lax.fori_loop(0, count, weigh, ((zeros, zeros),) * n)
        for (hi, slot), (total, summed) in zip(tasks, state):
            total = jnp.sum(total, axis=1, keepdims=True)
            rows = slice(slot * group, (slot + 1) * group)
            out_refs[hi][rows, :] = (summed / total).astype(jnp.bfloat16)

    for slot in range(2):
        for hi in range(0, n_hi, PAIR):
            attend([(hi + t, slot) for t in range(PAIR)])


def shards(n_blk, queries, keys, values, group_table, doc_ids):
    tok_rows = queries.shape[0]
    group = tok_rows // 2
    n_hi = queries.shape[1] // HEAD_DIM
    n_lo = n_blk // n_hi
    seq = doc_ids.shape[0]
    assert seq // group <= 256
    me = lax.axis_index("blk")
    my_hi = me // n_lo

    def swap(x, by):
        return lax.ppermute(x, "blk", [(b, b ^ by) for b in range(n_blk)])

    def head_of(x, hi):
        return lax.dynamic_slice(x, (0, hi * HEAD_DIM), (tok_rows, HEAD_DIM))

    notes = jnp.repeat(group_table[0], NOTE_ROWS // 2).astype(jnp.bfloat16)
    notes = jnp.broadcast_to(notes[:, None], (NOTE_ROWS, HEAD_DIM))
    kv_rows = 2 * tok_rows + NOTE_ROWS
    sends = []
    for step in range(n_hi):
        hi = my_hi ^ step
        sends.append(jnp.concatenate([head_of(keys, hi), head_of(values, hi), notes, head_of(queries, hi)]))
    first = n_lo // 2
    pieces = [swap(sends[step], step * n_lo) if step else sends[0] for step in range(n_hi)]
    across = [swap(sends[step][:kv_rows], step * n_lo + first) for step in range(2)]

    def gather(held, bit):
        while bit:
            for j in list(held):
                held[j ^ bit] = swap(held[j], bit)
            bit //= 2
        return [held[j] for j in range(1, n_lo)]

    near = jnp.stack([piece[:kv_rows] for piece in pieces[:2]])
    far = jnp.stack([piece[:kv_rows] for piece in pieces[2:]])
    batches = gather({0: near, first: jnp.stack(across)}, first // 2) + gather({0: far}, first)

    index = jnp.arange(seq, dtype=jnp.int32)
    before = jnp.concatenate([doc_ids[:1], doc_ids[:-1]])
    start = lax.cummax(jnp.where(doc_ids != before, index, 0))
    start = start.reshape(seq // group, group)

    smem = pl.BlockSpec(memory_space=pltpu.SMEM)
    vmem = pl.BlockSpec(memory_space=pltpu.VMEM)
    outs = pl.pallas_call(
        functools.partial(attend_kernel, n_hi, n_lo, group),
        out_shape=[jax.ShapeDtypeStruct((tok_rows, HEAD_DIM), jnp.bfloat16)] * n_hi,
        in_specs=[smem] + [vmem] * (1 + n_hi + 2 * (n_lo - 1)),
        out_specs=[vmem] * n_hi,
        scratch_shapes=[
            pltpu.VMEM((seq + CHUNK, HEAD_DIM), jnp.bfloat16),
            pltpu.VMEM((seq + CHUNK, HEAD_DIM), jnp.bfloat16),
            pltpu.VMEM((PAIR, seq // CHUNK, group, CHUNK), jnp.float32),
        ],
        name="attend",
    )(
        start[:, 0], start, *pieces, *batches,
    )
    back = jnp.stack([swap(outs[j], j * n_lo) if j else outs[0] for j in range(n_hi)])
    heads = [lax.dynamic_index_in_dim(back, my_hi ^ h, 0, keepdims=False) for h in range(n_hi)]
    return jnp.concatenate(heads, axis=1)


def solution(mesh):
    in_specs = (P("blk", "head"), P("blk", "head"), P("blk", "head"), P("blk", None), P())
    out_specs = P("blk", "head")
    body = functools.partial(shards, mesh.shape["blk"])
    return jax.shard_map(body, mesh=mesh, in_specs=in_specs, out_specs=out_specs, check_vma=False)
```
